32 devices in a mesh: lat: 2 (over core), lon: 4 (over y, x), lev: 4 (over z).
Axes of the slice: x: 2, y: 2, z: 4, core: 2. Of those that a mesh axis runs over, the one named last changes fastest.
Arguments:
- field_values: float32 [16, 512, 64, 128], P('lat', 'lon', 'lev'), may hold values from 0.2 to 1.8
- crowding: float32 [16, 512, 64, 128], P('lat', 'lon', 'lev'), may hold values from 0.5 to 2
Outputs:
- potential: float32 [16, 512, 64, 128], P('lat', 'lon', 'lev')
- field_values_end: float32 [16, 512, 64, 128], P('lat', 'lon', 'lev')
The draws below stay inside these ranges and needn't reach their ends.
All inputs are finite; a program needn't handle non-finite values.
Results may differ from the reference program's by a relative error of at most 0.00002.
Values sent between devices are 32-bit elements; how exact they have to be, the bound alone decides.
No kernel may reach another device: no remote copies, remote signals or barrier semaphores. Data moves between devices by JAX's collectives and lax.ppermute only.
A program may use at most 256 MiB of HBM per device.

```python
import jax
import jax.numpy as jnp
from jax import lax

GRID_Y = 16
GRID_X = 512
GRID_Z = 64
LEVELS = 128
STEPS = 4


def block_levels(rng, shape, split, low, top_value):
    def one(axis_at, parts):
        heights = jax.random.uniform(jax.random.fold_in(jax.random.fold_in(rng, 6), axis_at), (parts,), jnp.float32, low / len(split), top_value / len(split))
        return jnp.repeat(jnp.exp(heights), shape[axis_at] // parts).reshape((-1,) + (1,) * (len(shape) - axis_at - 1))

    gain = one(*split[0])
    for cut in split[1:]:
        gain = gain * one(*cut)
    return gain


def setup_inputs(seed: int = 0) -> dict:
    splits = jax.random.split(jax.random.key(seed), 3)
    field_values = jnp.clip(0.2 + 1.5999999 * jax.random.uniform(splits[0], (GRID_Y, GRID_X, GRID_Z, LEVELS), jnp.float32) ** block_levels(splits[0], (GRID_Y, GRID_X, GRID_Z, LEVELS), ((0, 2), (1, 4), (2, 4)), -0.2, 0.2), 0.2, 1.8)
    crowding = jnp.clip(0.5 + 1.5 * jax.random.uniform(splits[1], (GRID_Y, GRID_X, GRID_Z, LEVELS), jnp.float32) ** block_levels(splits[1], (GRID_Y, GRID_X, GRID_Z, LEVELS), ((0, 2), (1, 4), (2, 4)), -0.2, 0.2), 0.5, 2.0)
    return {"field_values": field_values, "crowding": crowding}


def without_rim(values, dims):
    for dim in dims:
        values = lax.slice_in_dim(values, 1, values.shape[dim] - 1, axis=dim)
    return values


def shifted_cells(values, dim, start, dims):
    others = [other for other in dims if other != dim]
    values = without_rim(values, others)
    return lax.slice_in_dim(values, start, start + values.shape[dim] - 2, axis=dim)


def march_step(padded, crowding):
    middle = without_rim(padded, (0, 1, 2))
    lower = [shifted_cells(padded, dim, 0, (0, 1, 2)) for dim in (0, 1, 2)]
    upper = [shifted_cells(padded, dim, 2, (0, 1, 2)) for dim in (0, 1, 2)]
    spread = lower[0] + upper[0] + lower[1] + upper[1] + lower[2] + upper[2] - 6.0 * middle
    return middle + 0.1 * spread + 0.2 * middle * (1.0 - middle * crowding)


def reference(field_values, crowding):
    for step in range(STEPS):
        field_values = march_step(jnp.pad(field_values, ((1, 1), (1, 1), (1, 1), (0, 0)), mode="wrap"), crowding)
    potential = jnp.cumsum(field_values, axis=2) / GRID_Z
    return potential, field_values
```

```python
import functools

import jax
import jax.numpy as jnp
from jax import lax
from jax.experimental import pallas as pl
from jax.experimental.pallas import tpu as pltpu
from jax.sharding import PartitionSpec as P

STEPS = 4
CHUNK = 16
PARTS = 2


def ups(count):
    return [(i, (i + 1) % count) for i in range(count)]


def downs(count):
    return [((i + 1) % count, i) for i in range(count)]


def add_faces(cells, low, high):
    depth = cells.shape[-2]
    layer = lax.broadcasted_iota(jnp.int32, cells.shape, cells.ndim - 2)
    cells = cells + jnp.where(layer == 0, jnp.expand_dims(low, -2), 0.0)
    return cells + jnp.where(layer == depth - 1, jnp.expand_dims(high, -2), 0.0)


def march_kernel(corrected, last, *refs):
    refs = list(refs)
    h_ref, prev_ref, next_ref = refs[:3]
    refs = refs[3:]
    if corrected:
        low_ref, high_ref = refs[:2]
        refs = refs[2:]
    xlow_ref, xhigh_ref, ylow_ref, yhigh_ref, c_ref = refs[:5]
    refs = refs[5:]
    out_ref = refs[0]
    held = refs[-1]
    rows, chunk, depth, lanes = h_ref.shape
    step = pl.program_id(0)
    steps = pl.num_programs(0)
    span = chunk * steps
    layer = lax.broadcasted_iota(jnp.int32, (depth, lanes), 0)
    first = layer == 0
    final = layer == depth - 1

    def fix(values, row, place):
        if not corrected:
            return values
        low = low_ref[row, pl.ds(place, 1), :]
        high = high_ref[row, pl.ds(place, 1), :]
        return values + jnp.where(first, low, 0.0) + jnp.where(final, high, 0.0)

    base = step * chunk

    def fill(at, _):
        held[0, at + 1] = ylow_ref[0, at]
        held[rows + 1, at + 1] = yhigh_ref[0, at]
        for row in range(rows):
            held[row + 1, at + 1] = fix(h_ref[row, at], row, base + at)
        return 0

    lax.fori_loop(0, chunk, fill, 0)

    @pl.when(step == 0)
    def _():
        for row in range(rows):
            held[row + 1, 0] = xlow_ref[row]

    @pl.when(step > 0)
    def _():
        for row in range(rows):
            held[row + 1, 0] = fix(prev_ref[row, 0], row, jnp.maximum(base - 1, 0))

    @pl.when(step == steps - 1)
    def _():
        for row in range(rows):
            held[row + 1, chunk + 1] = xhigh_ref[row]

    @pl.when(step < steps - 1)
    def _():
        for row in range(rows):
            held[row + 1, chunk + 1] = fix(next_ref[row, 0], row, jnp.minimum(base + chunk, span - 1))

    def march(at, _):
        for row in range(rows):
            mid = held[row + 1, at + 1]
            around = held[row, at + 1] + held[row + 2, at + 1] + held[row + 1, at] + held[row + 1, at + 2]
            around = around + jnp.where(first, 0.0, pltpu.roll(mid, 1, 0))
            around = around + jnp.where(final, 0.0, pltpu.roll(mid, depth - 1, 0))
            new = mid * (0.6 - 0.2 * (mid * c_ref[row, at])) + 0.1 * around
            out_ref[row, at] = new
            if last:
                refs[1][row, pl.ds(at, 1), :] = jnp.sum(new, axis=0, keepdims=True)
            else:
                refs[1][row, pl.ds(at, 1), :] = new[:1]
                refs[2][row, pl.ds(at, 1), :] = new[depth - 1 :]
        return 0

    lax.fori_loop(0, chunk, march, 0)


def march(h, faces, xlow, xhigh, ylow, yhigh, crowding, last):
    rows, span, depth, lanes = h.shape
    chunk = CHUNK
    steps = span // chunk
    whole = pl.BlockSpec((rows, chunk, depth, lanes), lambda i: (0, i, 0, 0))
    flat = pl.BlockSpec((rows, chunk, lanes), lambda i: (0, i, 0))
    face = pl.BlockSpec((rows, span, lanes), lambda i: (0, 0, 0))
    edge = pl.BlockSpec((rows, depth, lanes), lambda i: (0, 0, 0))
    specs = [
        whole,
        pl.BlockSpec((rows, 1, depth, lanes), lambda i: (0, jnp.maximum(i * chunk - 1, 0), 0, 0)),
        pl.BlockSpec((rows, 1, depth, lanes), lambda i: (0, jnp.minimum(i * chunk + chunk, span - 1), 0, 0)),
    ]
    operands = [h, h, h]
    if faces is not None:
        specs += [face, face]
        operands += list(faces)
    specs += [edge, edge]
    operands += [xlow, xhigh]
    for array, index in (ylow, yhigh):
        specs.append(pl.BlockSpec((1, chunk, depth, lanes), functools.partial(lambda k, i: (k, i, 0, 0), index)))
        operands.append(array)
    specs.append(whole)
    operands.append(crowding)
    flats = jax.ShapeDtypeStruct((rows, span, lanes), h.dtype)
    count = 1 if last else 2
    return pl.pallas_call(
        functools.partial(march_kernel, faces is not None, last),
        grid=(steps,),
        in_specs=specs,
        out_specs=[whole] + [flat] * count,
        out_shape=[jax.ShapeDtypeStruct(h.shape, h.dtype)] + [flats] * count,
        scratch_shapes=[pltpu.VMEM((rows + 2, chunk + 2, depth, lanes), h.dtype)],
        compiler_params=pltpu.CompilerParams(vmem_limit_bytes=24 * 1024 * 1024),
        cost_estimate=pl.CostEstimate(flops=16 * h.size, bytes_accessed=13 * h.size, transcendentals=0),
        name="march",
    )(*operands)


def finish_kernel(scale, h_ref, low_ref, high_ref, below_ref, pot_ref, end_ref):
    rows, chunk, depth, lanes = h_ref.shape
    layer = lax.broadcasted_iota(jnp.int32, (depth, lanes), 0)

    def one(at, _):
        for row in range(rows):
            low = low_ref[row, pl.ds(at, 1), :]
            high = high_ref[row, pl.ds(at, 1), :]
            below = below_ref[row, pl.ds(at, 1), :]
            cells = h_ref[row, at] + jnp.where(layer == 0, low, 0.0) + jnp.where(layer == depth - 1, high, 0.0)
            end_ref[row, at] = cells
            total = cells
            shift = 1
            while shift < depth:
                total = total + jnp.where(layer >= shift, pltpu.roll(total, shift, 0), 0.0)
                shift *= 2
            pot_ref[row, at] = (total + below) * scale
        return 0

    lax.fori_loop(0, chunk, one, 0)


def finish(h, low, high, below, scale):
    rows, span, depth, lanes = h.shape
    chunk = CHUNK
    whole = pl.BlockSpec((rows, chunk, depth, lanes), lambda i: (0, i, 0, 0))
    flat = pl.BlockSpec((rows, chunk, lanes), lambda i: (0, i, 0))
    return pl.pallas_call(
        functools.partial(finish_kernel, scale),
        grid=(span // chunk,),
        in_specs=[whole, flat, flat, flat],
        out_specs=[whole, whole],
        out_shape=[jax.ShapeDtypeStruct(h.shape, h.dtype)] * 2,
        compiler_params=pltpu.CompilerParams(vmem_limit_bytes=24 * 1024 * 1024),
        cost_estimate=pl.CostEstimate(flops=16 * h.size, bytes_accessed=13 * h.size, transcendentals=0),
        name="finish",
    )(h, low, high, below)


def side_halos(h, faces):
    rows, span = h.shape[:2]
    lats, lons = lax.axis_size("lat"), lax.axis_size("lon")

    def edge(y=None, x=None):
        pick = (lambda a: a[y]) if x is None else (lambda a: a[:, x])
        cells = pick(h)
        return cells if faces is None else add_faces(cells, pick(faces[0]), pick(faces[1]))

    both = jnp.stack([edge(y=0), edge(y=rows - 1)])
    if lats == 2:
        swapped = lax.ppermute(both, "lat", [(0, 1), (1, 0)])
        ylow, yhigh = (swapped, 1), (swapped, 0)
    else:
        ylow = (lax.ppermute(both[1:], "lat", ups(lats)), 0)
        yhigh = (lax.ppermute(both[:1], "lat", downs(lats)), 0)
    xlow = lax.ppermute(edge(x=span - 1), "lon", ups(lons))
    xhigh = lax.ppermute(edge(x=0), "lon", downs(lons))
    return xlow, xhigh, ylow, yhigh


def per_device(field, crowding):
    levs = lax.axis_size("lev")
    depth = field.shape[2]
    h = field
    low, high = field[:, :, 0], field[:, :, depth - 1]
    faces = None
    for step in range(STEPS):
        last = step == STEPS - 1
        above = lax.ppermute(low, "lev", downs(levs))
        below = lax.ppermute(high, "lev", ups(levs))
        halos = side_halos(h, faces)
        outs = march(h, faces, *halos, crowding, last)
        h = outs[0]
        faces = (0.1 * below, 0.1 * above)
        if not last:
            low = outs[1] + faces[0]
            high = outs[2] + faces[1]
    total = outs[1] + faces[0] + faces[1]
    rows = total.shape[0]
    parts = []
    for part in range(PARTS):
        mine = total[part * rows // PARTS : (part + 1) * rows // PARTS]
        before = jnp.zeros_like(mine)
        for hop in range(levs - 1):
            before = before + lax.ppermute(before + mine, "lev", [(hop, hop + 1)])
        parts.append(before)
    before = jnp.concatenate(parts, axis=0)
    return finish(h, faces[0], faces[1], before, 1.0 / (depth * levs))


def solution(mesh):
    return jax.shard_map(
        per_device,
        mesh=mesh,
        in_specs=(P("lat", "lon", "lev", None), P("lat", "lon", "lev", None)),
        out_specs=(P("lat", "lon", "lev", None), P("lat", "lon", "lev", None)),
        check_vma=False,
    )
```

```python
import functools

import jax
import jax.numpy as jnp
from jax import lax
from jax.experimental import pallas as pl
from jax.experimental.pallas import tpu as pltpu
from jax.sharding import PartitionSpec as P

STEPS = 4
TILE = 8
PARTS = 2
MIB = 1024 * 1024


CHUNKS = 8
VMEM = pl.BlockSpec(memory_space=pltpu.VMEM)
HBM = pl.BlockSpec(memory_space=pltpu.HBM)


def ups(count):
    return [(i, (i + 1) % count) for i in range(count)]


def downs(count):
    return [((i + 1) % count, i) for i in range(count)]


def like(shape, array):
    return jax.ShapeDtypeStruct(shape, array.dtype)


def add_faces(cells, low, high):
    depth = cells.shape[-2]
    layer = lax.broadcasted_iota(jnp.int32, cells.shape, cells.ndim - 2)
    cells = jnp.where(layer == 0, jnp.expand_dims(low, -2), cells)
    return jnp.where(layer == depth - 1, jnp.expand_dims(high, -2), cells)


def peel_kernel(f_ref, h_ref, low_ref, high_ref, both_ref, first_ref, final_ref, ground_ref, sems):
    ground_ref[...] = jnp.full(ground_ref.shape, jnp.where(lax.axis_index("lev") == 0, 1.0, 0.0), ground_ref.dtype)
    rows, span, depth, _ = h_ref.shape
    chunk = span // CHUNKS
    copies = []
    for k in range(CHUNKS):
        part = pl.ds(k * chunk, chunk)
        copies.append(pltpu.make_async_copy(f_ref.at[:, part], h_ref.at[:, part], sems.at[k]))
        copies[-1].start()

    def one(at, _):
        for row in range(rows):
            low_ref[row, pl.ds(at, 1), :] = h_ref[row, at, pl.ds(0, 1), :]
            high_ref[row, pl.ds(at, 1), :] = h_ref[row, at, pl.ds(depth - 1, 1), :]
        both_ref[0, at] = h_ref[0, at]
        both_ref[1, at] = h_ref[rows - 1, at]
        return 0

    for k in range(CHUNKS):
        copies[k].wait()
        lax.fori_loop(k * chunk, (k + 1) * chunk, one, 0)
    for row in range(rows):
        first_ref[row] = h_ref[row, 0]
        final_ref[row] = h_ref[row, span - 1]


def peel(field):
    rows, span, depth, lanes = field.shape
    face = like((rows, span, lanes), field)
    edge = like((rows, depth, lanes), field)
    return pl.pallas_call(
        peel_kernel,
        in_specs=[HBM],
        out_specs=[VMEM] * 7,
        out_shape=[like(field.shape, field), face, face, like((2, span, depth, lanes), field), edge, edge, like((1, 1, lanes), field)],
        scratch_shapes=[pltpu.SemaphoreType.DMA((CHUNKS,))],
        compiler_params=pltpu.CompilerParams(vmem_limit_bytes=2 * MIB),
        cost_estimate=pl.CostEstimate(flops=4 * field.size, bytes_accessed=field.size, transcendentals=0),
        name="peel",
    )(field)


def march_kernel(fixed, last, ylow_at, yhigh_at, *refs):
    refs = list(refs)
    h_ref = refs.pop(0)
    low_ref, high_ref = (refs.pop(0), refs.pop(0)) if fixed else (None, None)
    xlow_ref, xhigh_ref, ylow_ref, yhigh_ref, c_ref, out_ref = refs[:6]
    refs = refs[6:]
    rows, span, depth, lanes = h_ref.shape
    tiles = depth // TILE
    sub = lax.broadcasted_iota(jnp.int32, (TILE, lanes), 0)
    first, final = sub == 0, sub == TILE - 1

    def tile(t):
        return pl.ds(t * TILE, TILE)

    def cells_at(at):
        out = []
        for row in range(rows):
            cells = [h_ref[row, at, tile(t), :] for t in range(tiles)]
            if fixed:
                cells[0] = jnp.where(first, low_ref[row, pl.ds(at, 1), :], cells[0])
                cells[-1] = jnp.where(final, high_ref[row, pl.ds(at, 1), :], cells[-1])
            out.append(cells)
        return out

    def edge(ref):
        return [[ref[row, tile(t), :] for t in range(tiles)] for row in range(rows)]

    def one(at, before, here, after):
        for row in range(rows):
            mids = here[row]
            down = [pltpu.roll(m, 1, 0) for m in mids]
            up = [pltpu.roll(m, TILE - 1, 0) for m in mids]
            news = []
            for t in range(tiles):
                ylow = ylow_ref[ylow_at, at, tile(t), :] if row == 0 else here[row - 1][t]
                yhigh = yhigh_ref[yhigh_at, at, tile(t), :] if row == rows - 1 else here[row + 1][t]
                around = (ylow + yhigh) + (before[row][t] + after[row][t])
                around = around + jnp.where(first, down[t - 1] if t else 0.0, down[t])
                around = around + jnp.where(final, up[t + 1] if t < tiles - 1 else 0.0, up[t])
                mid = mids[t]
                new = mid * (0.6 - 0.2 * (mid * c_ref[row, at, tile(t), :])) + 0.1 * around
                out_ref[row, at, tile(t), :] = new
                news.append(new)
            if last:
                total = functools.reduce(jnp.add, news)
                refs[0][row, pl.ds(at, 1), :] = jnp.sum(total, axis=0, keepdims=True)
            else:
                refs[0][row, pl.ds(at, 1), :] = news[0][:1]
                refs[1][row, pl.ds(at, 1), :] = news[-1][TILE - 1 :]

    def step(at, carry):
        before, here = carry
        after = cells_at(at + 1)
        one(at, before, here, after)
        return here, after

    before, here = lax.fori_loop(0, span - 1, step, (edge(xlow_ref), cells_at(0)))
    one(span - 1, before, here, edge(xhigh_ref))


def march(h, faces, xlow, xhigh, ylow, yhigh, crowding, last):
    rows, span, _, lanes = h.shape
    face = like((rows, span, lanes), h)
    count = 1 if last else 2
    operands = [h, *(faces or ()), xlow, xhigh, ylow[0], yhigh[0], crowding]
    return pl.pallas_call(
        functools.partial(march_kernel, faces is not None, last, ylow[1], yhigh[1]),
        in_specs=[VMEM] * len(operands),
        out_specs=[VMEM] * (1 + count),
        out_shape=[like(h.shape, h)] + [face] * count,
        input_output_aliases={0: 0},
        compiler_params=pltpu.CompilerParams(vmem_limit_bytes=2 * MIB),
        cost_estimate=pl.CostEstimate(flops=16 * h.size, bytes_accessed=12 * h.size, transcendentals=0),
        name="march",
    )(*operands)


def end_kernel(h_ref, low_ref, high_ref, end_ref, sum_ref, stage, sems):
    rows, span, depth, lanes = h_ref.shape
    tiles = depth // TILE
    chunk = span // CHUNKS
    sub = lax.broadcasted_iota(jnp.int32, (TILE, lanes), 0)

    def copy(k):
        return pltpu.make_async_copy(stage.at[k % 2], end_ref.at[:, pl.ds(k * chunk, chunk)], sems.at[k])

    for k in range(CHUNKS):
        if k >= 2:
            copy(k - 2).wait()

        def one(step, _):
            at = step + k * chunk
            held = [[h_ref[row, at, pl.ds(t * TILE, TILE), :] for t in range(tiles)] for row in range(rows)]
            for row in range(rows):
                carry = None
                for t in range(tiles):
                    part = pl.ds(t * TILE, TILE)
                    cells = held[row][t]
                    end = cells
                    if t == 0:
                        end = end + jnp.where(sub == 0, low_ref[row, pl.ds(at, 1), :], 0.0)
                    if t == tiles - 1:
                        end = end + jnp.where(sub == TILE - 1, high_ref[row, pl.ds(at, 1), :], 0.0)
                    stage[k % 2, row, step, part, :] = end
                    shift = 1
                    while shift < TILE:
                        cells = cells + jnp.where(sub >= shift, pltpu.roll(cells, shift, 0), 0.0)
                        shift *= 2
                    held[row][t] = cells if carry is None else cells + carry
                    carry = held[row][t][TILE - 1 :]
            for row in range(rows):
                for t in range(tiles):
                    sum_ref[row, at, pl.ds(t * TILE, TILE), :] = held[row][t]
            return 0

        lax.fori_loop(0, chunk, one, 0)
        copy(k).start()
    for k in (CHUNKS - 2, CHUNKS - 1):
        copy(k).wait()


def end(h, low, high):
    rows, span, depth, lanes = h.shape
    return pl.pallas_call(
        end_kernel,
        in_specs=[VMEM] * 3,
        out_specs=[HBM, VMEM],
        out_shape=[like(h.shape, h)] * 2,
        scratch_shapes=[pltpu.VMEM((2, rows, span // CHUNKS, depth, lanes), h.dtype), pltpu.SemaphoreType.DMA((CHUNKS,))],
        input_output_aliases={0: 1},
        compiler_params=pltpu.CompilerParams(vmem_limit_bytes=4 * MIB),
        cost_estimate=pl.CostEstimate(flops=12 * h.size, bytes_accessed=12 * h.size, transcendentals=0),
        name="end",
    )(h, low, high)


def potential_kernel(scale, offset, sum_ref, prior_ref, got_ref, rest_ref, high_ref, *refs):
    pot_ref, stage, sems = refs[-3:]
    rows, span, depth, lanes = stage.shape
    chunk = span // CHUNKS
    layer = lax.broadcasted_iota(jnp.int32, (depth, lanes), 0)

    def one(at, _):
        for row in range(rows):
            base = prior_ref[row, pl.ds(at, 1), :] + got_ref[row, pl.ds(at, 1), :]
            base = base + rest_ref[row + offset, pl.ds(at, 1), :]
            high = high_ref[row + offset, pl.ds(at, 1), :]
            cells = sum_ref[row + offset, at] + base
            stage[row, at] = (cells + jnp.where(layer == depth - 1, high, 0.0)) * scale
        return 0

    copies = []
    for k in range(CHUNKS):
        lax.fori_loop(k * chunk, (k + 1) * chunk, one, 0)
        part = pl.ds(k * chunk, chunk)
        copies.append(pltpu.make_async_copy(stage.at[:, part], pot_ref.at[pl.ds(offset, rows), part], sems.at[k]))
        copies[-1].start()
    for copy in copies:
        copy.wait()


def potential(sums, prior, got, rest, high, scale, part, made):
    _, span, depth, lanes = sums.shape
    some = got.shape[0]
    return pl.pallas_call(
        functools.partial(potential_kernel, scale, part * some),
        in_specs=[VMEM] * 5 + ([] if made is None else [HBM]),
        out_specs=HBM,
        out_shape=like(sums.shape, sums),
        scratch_shapes=[pltpu.VMEM((some, span, depth, lanes), sums.dtype), pltpu.SemaphoreType.DMA((CHUNKS,))],
        input_output_aliases={} if made is None else {5: 0},
        compiler_params=pltpu.CompilerParams(vmem_limit_bytes=(2 + 8 // PARTS) * MIB),
        cost_estimate=pl.CostEstimate(flops=2 * sums.size, bytes_accessed=8 * sums.size // PARTS, transcendentals=0),
        name="potential",
    )(sums, prior, got, rest, high, *(() if made is None else (made,)))


def side_halos(both, first, final):
    lats, lons = lax.axis_size("lat"), lax.axis_size("lon")
    if lats == 2:
        swapped = lax.ppermute(both, "lat", [(0, 1), (1, 0)])
        ylow, yhigh = (swapped, 1), (swapped, 0)
    else:
        ylow = (lax.ppermute(both[1:], "lat", ups(lats)), 0)
        yhigh = (lax.ppermute(both[:1], "lat", downs(lats)), 0)
    xlow = lax.ppermute(final, "lon", ups(lons))
    xhigh = lax.ppermute(first, "lon", downs(lons))
    return xlow, xhigh, ylow, yhigh


def edges(h, low, high):
    rows, span = h.shape[:2]
    both = jnp.stack([add_faces(h[y], low[y], high[y]) for y in (0, rows - 1)])
    first, final = (add_faces(h[:, x], low[:, x], high[:, x]) for x in (0, span - 1))
    return both, first, final


def steps(field, crowding):
    levs = lax.axis_size("lev")
    depth = field.shape[2]
    faces = None
    h, low, high, both, first, final, ground = peel(field)
    for step in range(STEPS):
        last = step == STEPS - 1
        above = lax.ppermute(low, "lev", downs(levs))
        below = lax.ppermute(high, "lev", ups(levs))
        halos = side_halos(both, first, final)
        outs = march(h, faces, *halos, crowding, last)
        h = outs[0]
        if not last:
            low = outs[1] + 0.1 * below
            high = outs[2] + 0.1 * above
            faces = (low, high)
            both, first, final = edges(h, low, high)
    rest = 0.1 * jnp.where(ground > 0.0, below, low)
    own = outs[1] + 0.1 * high + rest
    top = 0.1 * above
    field_end, sums = end(h, 0.1 * below, top)
    rows = own.shape[0] // PARTS
    made = None
    for part in range(PARTS):
        mine = own[part * rows : (part + 1) * rows]
        before, got = jnp.zeros_like(mine), jnp.zeros_like(mine)
        for hop in range(levs - 1):
            before = before + got
            got = lax.ppermute(before + mine, "lev", [(hop, hop + 1)])
        made = potential(sums, before, got, rest, top, 1.0 / (depth * levs), part, made)
    return made, field_end


def solution(mesh):
    return jax.shard_map(
        steps,
        mesh=mesh,
        in_specs=(P("lat", "lon", "lev", None), P("lat", "lon", "lev", None)),
        out_specs=(P("lat", "lon", "lev", None), P("lat", "lon", "lev", None)),
        check_vma=False,
    )
```

```python
import functools

import jax
import jax.numpy as jnp
from jax import lax
from jax.experimental import pallas as pl
from jax.experimental.pallas import tpu as pltpu
from jax.sharding import PartitionSpec as P

STEPS = 4
TILE = 8
PARTS = 4
MIB = 1024 * 1024


CHUNKS = 8
SLOTS = 4
VMEM = pl.BlockSpec(memory_space=pltpu.VMEM)
HBM = pl.BlockSpec(memory_space=pltpu.HBM)


def ups(count):
    return [(i, (i + 1) % count) for i in range(count)]


def downs(count):
    return [((i + 1) % count, i) for i in range(count)]


def like(shape, array):
    return jax.ShapeDtypeStruct(shape, array.dtype)


def add_faces(cells, low, high):
    depth = cells.shape[-2]
    layer = lax.broadcasted_iota(jnp.int32, cells.shape, cells.ndim - 2)
    cells = jnp.where(layer == 0, jnp.expand_dims(low, -2), cells)
    return jnp.where(layer == depth - 1, jnp.expand_dims(high, -2), cells)


def peel_kernel(f_ref, h_ref, low_ref, high_ref, both_ref, first_ref, final_ref, ground_ref, sems):
    ground_ref[...] = jnp.full(ground_ref.shape, jnp.where(lax.axis_index("lev") == 0, 1.0, 0.0), ground_ref.dtype)
    rows, span, depth, _ = h_ref.shape
    chunk = span // CHUNKS
    copies = []
    for k in range(CHUNKS):
        part = pl.ds(k * chunk, chunk)
        copies.append(pltpu.make_async_copy(f_ref.at[:, part], h_ref.at[:, part], sems.at[k]))
        copies[-1].start()

    def one(at, _):
        for row in range(rows):
            low_ref[row, pl.ds(at, 1), :] = h_ref[row, at, pl.ds(0, 1), :]
            high_ref[row, pl.ds(at, 1), :] = h_ref[row, at, pl.ds(depth - 1, 1), :]
        both_ref[0, at] = h_ref[0, at]
        both_ref[1, at] = h_ref[rows - 1, at]
        return 0

    for k in range(CHUNKS):
        copies[k].wait()
        lax.fori_loop(k * chunk, (k + 1) * chunk, one, 0, unroll=4)
    for row in range(rows):
        first_ref[row] = h_ref[row, 0]
        final_ref[row] = h_ref[row, span - 1]


def peel(field):
    rows, span, depth, lanes = field.shape
    face = like((rows, span, lanes), field)
    edge = like((rows, depth, lanes), field)
    return pl.pallas_call(
        peel_kernel,
        in_specs=[HBM],
        out_specs=[VMEM] * 7,
        out_shape=[like(field.shape, field), face, face, like((2, span, depth, lanes), field), edge, edge, like((1, 1, lanes), field)],
        scratch_shapes=[pltpu.SemaphoreType.DMA((CHUNKS,))],
        compiler_params=pltpu.CompilerParams(vmem_limit_bytes=42 * MIB),
        cost_estimate=pl.CostEstimate(flops=4 * field.size, bytes_accessed=field.size, transcendentals=0),
        name="peel",
    )(field)


def march_kernel(fixed, last, ylow_at, yhigh_at, *refs):
    refs = list(refs)
    h_ref = refs.pop(0)
    low_ref, high_ref = (refs.pop(0), refs.pop(0)) if fixed else (None, None)
    xlow_ref, xhigh_ref, ylow_ref, yhigh_ref, c_ref, out_ref = refs[:6]
    refs = refs[6:]
    rows, span, depth, lanes = h_ref.shape
    tiles = depth // TILE
    sub = lax.broadcasted_iota(jnp.int32, (TILE, lanes), 0)
    first, final = sub == 0, sub == TILE - 1

    def tile(t):
        return pl.ds(t * TILE, TILE)

    def cells_at(at):
        out = []
        for row in range(rows):
            cells = [h_ref[row, at, tile(t), :] for t in range(tiles)]
            if fixed:
                cells[0] = jnp.where(first, low_ref[row, pl.ds(at, 1), :], cells[0])
                cells[-1] = jnp.where(final, high_ref[row, pl.ds(at, 1), :], cells[-1])
            out.append(cells)
        return out

    def edge(ref):
        return [[ref[row, tile(t), :] for t in range(tiles)] for row in range(rows)]

    def one(at, before, here, after):
        for row in range(rows):
            mids = here[row]
            down = [pltpu.roll(m, 1, 0) for m in mids]
            up = [pltpu.roll(m, TILE - 1, 0) for m in mids]
            news = []
            for t in range(tiles):
                ylow = ylow_ref[ylow_at, at, tile(t), :] if row == 0 else here[row - 1][t]
                yhigh = yhigh_ref[yhigh_at, at, tile(t), :] if row == rows - 1 else here[row + 1][t]
                around = (ylow + yhigh) + (before[row][t] + after[row][t])
                around = around + jnp.where(first, down[t - 1] if t else 0.0, down[t])
                around = around + jnp.where(final, up[t + 1] if t < tiles - 1 else 0.0, up[t])
                mid = mids[t]
                new = mid * (0.6 - 0.2 * (mid * c_ref[row, at, tile(t), :])) + 0.1 * around
                out_ref[row, at, tile(t), :] = new
                news.append(new)
            if last:
                total = functools.reduce(jnp.add, news)
                refs[0][row, pl.ds(at, 1), :] = jnp.sum(total, axis=0, keepdims=True)
            else:
                refs[0][row, pl.ds(at, 1), :] = news[0][:1]
                refs[1][row, pl.ds(at, 1), :] = news[-1][TILE - 1 :]

    def step(at, carry):
        before, here = carry
        after = cells_at(at + 1)
        one(at, before, here, after)
        return here, after

    before, here = lax.fori_loop(0, span - 1, step, (edge(xlow_ref), cells_at(0)))
    one(span - 1, before, here, edge(xhigh_ref))


def march(h, faces, xlow, xhigh, ylow, yhigh, crowding, last):
    rows, span, _, lanes = h.shape
    face = like((rows, span, lanes), h)
    count = 1 if last else 2
    operands = [h, *(faces or ()), xlow, xhigh, ylow[0], yhigh[0], crowding]
    return pl.pallas_call(
        functools.partial(march_kernel, faces is not None, last, ylow[1], yhigh[1]),
        in_specs=[VMEM] * len(operands),
        out_specs=[VMEM] * (1 + count),
        out_shape=[like(h.shape, h)] + [face] * count,
        input_output_aliases={0: 0},
        compiler_params=pltpu.CompilerParams(vmem_limit_bytes=2 * MIB),
        cost_estimate=pl.CostEstimate(flops=16 * h.size, bytes_accessed=12 * h.size, transcendentals=0),
        name="march",
    )(*operands)


def sums_kernel(h_ref, sum_ref):
    rows, span, depth, lanes = h_ref.shape
    sub = lax.broadcasted_iota(jnp.int32, (TILE, lanes), 0)

    def one(at, _):
        for row in range(rows):
            carry = None
            for t in range(depth // TILE):
                cells = h_ref[row, at, pl.ds(t * TILE, TILE), :]
                shift = 1
                while shift < TILE:
                    cells = cells + jnp.where(sub >= shift, pltpu.roll(cells, shift, 0), 0.0)
                    shift *= 2
                cells = cells if carry is None else cells + carry
                sum_ref[row, at, pl.ds(t * TILE, TILE), :] = cells
                carry = cells[TILE - 1 :]
        return 0

    lax.fori_loop(0, span, one, 0, unroll=2)


def running_sums(h):
    return pl.pallas_call(
        sums_kernel,
        in_specs=[VMEM],
        out_specs=VMEM,
        out_shape=like(h.shape, h),
        compiler_params=pltpu.CompilerParams(vmem_limit_bytes=2 * MIB),
        cost_estimate=pl.CostEstimate(flops=8 * h.size, bytes_accessed=8 * h.size, transcendentals=0),
        name="sums",
    )(h)


def ending_kernel(h_ref, low_ref, high_ref, end_ref, stage, sems):
    rows, span, depth, lanes = h_ref.shape
    tiles = depth // TILE
    chunk = span // CHUNKS
    sub = lax.broadcasted_iota(jnp.int32, (TILE, lanes), 0)

    def copy(k):
        return pltpu.make_async_copy(stage.at[k % SLOTS], end_ref.at[:, pl.ds(k * chunk, chunk)], sems.at[k])

    for k in range(CHUNKS):
        if k >= SLOTS:
            copy(k - SLOTS).wait()

        def one(step, _):
            at = step + k * chunk
            for row in range(rows):
                for t in range(tiles):
                    cells = h_ref[row, at, pl.ds(t * TILE, TILE), :]
                    if t == 0:
                        cells = cells + jnp.where(sub == 0, low_ref[row, pl.ds(at, 1), :], 0.0)
                    if t == tiles - 1:
                        cells = cells + jnp.where(sub == TILE - 1, high_ref[row, pl.ds(at, 1), :], 0.0)
                    stage[k % SLOTS, row, step, pl.ds(t * TILE, TILE), :] = cells
            return 0

        lax.fori_loop(0, chunk, one, 0, unroll=2)
        copy(k).start()
    for k in range(CHUNKS - SLOTS, CHUNKS):
        copy(k).wait()


def ending(h, low, high):
    rows, span, depth, lanes = h.shape
    return pl.pallas_call(
        ending_kernel,
        in_specs=[VMEM] * 3,
        out_specs=HBM,
        out_shape=like(h.shape, h),
        scratch_shapes=[pltpu.VMEM((SLOTS, rows, span // CHUNKS, depth, lanes), h.dtype), pltpu.SemaphoreType.DMA((CHUNKS,))],
        compiler_params=pltpu.CompilerParams(vmem_limit_bytes=8 * MIB),
        cost_estimate=pl.CostEstimate(flops=2 * h.size, bytes_accessed=8 * h.size, transcendentals=0),
        name="ending",
    )(h, low, high)


def relay_kernel(offset, got_ref, *refs):
    prior_ref, (own_ref, before_ref, next_ref) = refs[0], refs[-3:]
    rows = got_ref.shape[0]
    before = got_ref[...] if len(refs) == 3 else prior_ref[...] + got_ref[...]
    before_ref[...] = before
    next_ref[...] = before + own_ref[pl.ds(offset, rows)]


def relay(prior, got, own, part):
    operands = [got] + ([] if prior is None else [prior]) + [own]
    return pl.pallas_call(
        functools.partial(relay_kernel, part * got.shape[0]),
        in_specs=[VMEM] * len(operands),
        out_specs=[VMEM] * 2,
        out_shape=[like(got.shape, got)] * 2,
        compiler_params=pltpu.CompilerParams(vmem_limit_bytes=2 * MIB),
        cost_estimate=pl.CostEstimate(flops=2 * got.size, bytes_accessed=16 * got.size, transcendentals=0),
        name="relay",
    )(*operands)


def potential_kernel(scale, offset, given, sum_ref, got_ref, rest_ref, high_ref, *refs):
    prior_ref = refs[0] if given else None
    pot_ref, stage, sems = refs[-3:]
    rows, span, depth, lanes = stage.shape
    chunk = span // CHUNKS
    layer = lax.broadcasted_iota(jnp.int32, (depth, lanes), 0)

    def one(at, _):
        for row in range(rows):
            base = got_ref[row, pl.ds(at, 1), :]
            base = base if prior_ref is None else base + prior_ref[row, pl.ds(at, 1), :]
            base = base + rest_ref[row + offset, pl.ds(at, 1), :]
            high = high_ref[row + offset, pl.ds(at, 1), :]
            cells = sum_ref[row + offset, at] + base
            stage[row, at] = (cells + jnp.where(layer == depth - 1, high, 0.0)) * scale
        return 0

    copies = []
    for k in range(CHUNKS):
        lax.fori_loop(k * chunk, (k + 1) * chunk, one, 0, unroll=4)
        part = pl.ds(k * chunk, chunk)
        copies.append(pltpu.make_async_copy(stage.at[:, part], pot_ref.at[pl.ds(offset, rows), part], sems.at[k]))
        copies[-1].start()
    for copy in copies:
        copy.wait()


def potential(sums, prior, got, rest, high, scale, part, made):
    _, span, depth, lanes = sums.shape
    some = got.shape[0]
    operands = [sums, got, rest, high] + ([] if prior is None else [prior])
    return pl.pallas_call(
        functools.partial(potential_kernel, scale, part * some, prior is not None),
        in_specs=[VMEM] * len(operands) + [HBM] * (made is not None),
        out_specs=HBM,
        out_shape=like(sums.shape, sums),
        scratch_shapes=[pltpu.VMEM((some, span, depth, lanes), sums.dtype), pltpu.SemaphoreType.DMA((CHUNKS,))],
        input_output_aliases={} if made is None else {len(operands): 0},
        compiler_params=pltpu.CompilerParams(vmem_limit_bytes=(2 + 8 // PARTS) * MIB),
        cost_estimate=pl.CostEstimate(flops=2 * sums.size, bytes_accessed=8 * sums.size // PARTS, transcendentals=0),
        name="potential",
    )(*operands, *(() if made is None else (made,)))


def side_halos(both, first, final):
    lats, lons = lax.axis_size("lat"), lax.axis_size("lon")
    if lats == 2:
        swapped = lax.ppermute(both, "lat", [(0, 1), (1, 0)])
        ylow, yhigh = (swapped, 1), (swapped, 0)
    else:
        ylow = (lax.ppermute(both[1:], "lat", ups(lats)), 0)
        yhigh = (lax.ppermute(both[:1], "lat", downs(lats)), 0)
    xlow = lax.ppermute(final, "lon", ups(lons))
    xhigh = lax.ppermute(first, "lon", downs(lons))
    return xlow, xhigh, ylow, yhigh


def edges(h, low, high):
    rows, span = h.shape[:2]
    both = jnp.stack([add_faces(h[y], low[y], high[y]) for y in (0, rows - 1)])
    first, final = (add_faces(h[:, x], low[:, x], high[:, x]) for x in (0, span - 1))
    return both, first, final


def steps(field, crowding):
    levs = lax.axis_size("lev")
    depth = field.shape[2]
    faces = None
    h, low, high, both, first, final, ground = peel(field)
    for step in range(STEPS):
        last = step == STEPS - 1
        above = lax.ppermute(low, "lev", downs(levs))
        below = lax.ppermute(high, "lev", ups(levs))
        halos = side_halos(both, first, final)
        outs = march(h, faces, *halos, crowding, last)
        h = outs[0]
        if not last:
            low = outs[1] + 0.1 * below
            high = outs[2] + 0.1 * above
            faces = (low, high)
            both, first, final = edges(h, low, high)
    rest = 0.1 * jnp.where(ground > 0.0, below, low)
    own = outs[1] + 0.1 * high + rest
    top = 0.1 * above
    sums = running_sums(h)
    field_end = ending(h, 0.1 * below, top)
    rows = own.shape[0] // PARTS
    nexts = [own[part * rows : (part + 1) * rows] for part in range(PARTS)]
    befores, gots = [None] * PARTS, [jnp.zeros_like(one) for one in nexts]
    for hop in range(levs - 1):
        for part in range(PARTS):
            if hop:
                befores[part], nexts[part] = relay(befores[part], gots[part], own, part)
            gots[part] = lax.ppermute(nexts[part], "lev", [(hop, hop + 1)])
    made = None
    for part in range(PARTS):
        made = potential(sums, befores[part], gots[part], rest, top, 1.0 / (depth * levs), part, made)
    return made, field_end


def solution(mesh):
    return jax.shard_map(
        steps,
        mesh=mesh,
        in_specs=(P("lat", "lon", "lev", None), P("lat", "lon", "lev", None)),
        out_specs=(P("lat", "lon", "lev", None), P("lat", "lon", "lev", None)),
        check_vma=False,
    )
```

```python
import functools

import jax
import jax.numpy as jnp
from jax import lax
from jax.experimental import pallas as pl
from jax.experimental.pallas import tpu as pltpu
from jax.sharding import PartitionSpec as P

STEPS = 4
TILE = 8
PARTS = 4
MIB = 1024 * 1024


CHUNKS = 8
GRANT = 40
SLOTS = 4
VMEM = pl.BlockSpec(memory_space=pltpu.VMEM)
HBM = pl.BlockSpec(memory_space=pltpu.HBM)


def ups(count):
    return [(i, (i + 1) % count) for i in range(count)]


def downs(count):
    return [((i + 1) % count, i) for i in range(count)]


def like(shape, array):
    return jax.ShapeDtypeStruct(shape, array.dtype)


def add_faces(cells, low, high):
    depth = cells.shape[-2]
    layer = lax.broadcasted_iota(jnp.int32, cells.shape, cells.ndim - 2)
    cells = jnp.where(layer == 0, jnp.expand_dims(low, -2), cells)
    return jnp.where(layer == depth - 1, jnp.expand_dims(high, -2), cells)


def layers_kernel(f_ref, low_ref, high_ref, sems):
    rows, _, depth, _ = f_ref.shape
    copies = []
    for side, (layer, face_ref) in enumerate(((0, low_ref), (depth - 1, high_ref))):
        for row in range(rows):
            copies.append(pltpu.make_async_copy(f_ref.at[row, :, layer], face_ref.at[row], sems.at[side, row]))
            copies[-1].start()
    for copy in copies:
        copy.wait()


def layers(field):
    rows, span, _, lanes = field.shape
    return pl.pallas_call(
        layers_kernel,
        in_specs=[HBM],
        out_specs=[VMEM] * 2,
        out_shape=[like((rows, span, lanes), field)] * 2,
        scratch_shapes=[pltpu.SemaphoreType.DMA((2, rows))],
        compiler_params=pltpu.CompilerParams(vmem_limit_bytes=50 * MIB),
        cost_estimate=pl.CostEstimate(flops=field.size, bytes_accessed=field.size, transcendentals=0),
        name="layers",
    )(field)


def peel_kernel(f_ref, h_ref, both_ref, first_ref, final_ref, ground_ref, sems):
    ground_ref[...] = jnp.full(ground_ref.shape, jnp.where(lax.axis_index("lev") == 0, 1.0, 0.0), ground_ref.dtype)
    rows, span, _, _ = h_ref.shape
    chunk = span // CHUNKS
    copies = []
    for k in range(CHUNKS):
        part = pl.ds(k * chunk, chunk)
        copies.append(pltpu.make_async_copy(f_ref.at[:, part], h_ref.at[:, part], sems.at[k]))
        copies[-1].start()

    def one(at, _):
        both_ref[0, at] = h_ref[0, at]
        both_ref[1, at] = h_ref[rows - 1, at]
        return 0

    for k in range(CHUNKS):
        copies[k].wait()
        lax.fori_loop(k * chunk, (k + 1) * chunk, one, 0, unroll=4)
    for row in range(rows):
        first_ref[row] = h_ref[row, 0]
        final_ref[row] = h_ref[row, span - 1]


def peel(field):
    rows, span, depth, lanes = field.shape
    edge = like((rows, depth, lanes), field)
    return pl.pallas_call(
        peel_kernel,
        in_specs=[HBM],
        out_specs=[VMEM] * 5,
        out_shape=[like(field.shape, field), like((2, span, depth, lanes), field), edge, edge, like((1, 1, lanes), field)],
        scratch_shapes=[pltpu.SemaphoreType.DMA((CHUNKS,))],
        compiler_params=pltpu.CompilerParams(vmem_limit_bytes=GRANT * MIB),
        cost_estimate=pl.CostEstimate(flops=4 * field.size, bytes_accessed=field.size, transcendentals=0),
        name="peel",
    )(field)


def march_kernel(fixed, last, ylow_at, yhigh_at, *refs):
    refs = list(refs)
    h_ref = refs.pop(0)
    low_ref, high_ref = (refs.pop(0), refs.pop(0)) if fixed else (None, None)
    xlow_ref, xhigh_ref, ylow_ref, yhigh_ref, c_ref, out_ref = refs[:6]
    refs = refs[6:]
    rows, span, depth, lanes = h_ref.shape
    tiles = depth // TILE
    sub = lax.broadcasted_iota(jnp.int32, (TILE, lanes), 0)
    first, final = sub == 0, sub == TILE - 1

    def tile(t):
        return pl.ds(t * TILE, TILE)

    def cells_at(at):
        out = []
        for row in range(rows):
            cells = [h_ref[row, at, tile(t), :] for t in range(tiles)]
            if fixed:
                cells[0] = jnp.where(first, low_ref[row, pl.ds(at, 1), :], cells[0])
                cells[-1] = jnp.where(final, high_ref[row, pl.ds(at, 1), :], cells[-1])
            out.append(cells)
        return out

    def edge(ref):
        return [[ref[row, tile(t), :] for t in range(tiles)] for row in range(rows)]

    def one(at, before, here, after):
        for row in range(rows):
            mids = here[row]
            down = [pltpu.roll(m, 1, 0) for m in mids]
            up = [pltpu.roll(m, TILE - 1, 0) for m in mids]
            news = []
            for t in range(tiles):
                ylow = ylow_ref[ylow_at, at, tile(t), :] if row == 0 else here[row - 1][t]
                yhigh = yhigh_ref[yhigh_at, at, tile(t), :] if row == rows - 1 else here[row + 1][t]
                around = (ylow + yhigh) + (before[row][t] + after[row][t])
                around = around + jnp.where(first, down[t - 1] if t else 0.0, down[t])
                around = around + jnp.where(final, up[t + 1] if t < tiles - 1 else 0.0, up[t])
                mid = mids[t]
                new = mid * (0.6 - 0.2 * (mid * c_ref[row, at, tile(t), :])) + 0.1 * around
                out_ref[row, at, tile(t), :] = new
                news.append(new)
            if last:
                total = functools.reduce(jnp.add, news)
                refs[0][row, pl.ds(at, 1), :] = jnp.sum(total, axis=0, keepdims=True)
            else:
                refs[0][row, pl.ds(at, 1), :] = news[0][:1]
                refs[1][row, pl.ds(at, 1), :] = news[-1][TILE - 1 :]

    def step(at, carry):
        before, here = carry
        after = cells_at(at + 1)
        one(at, before, here, after)
        return here, after

    before, here = lax.fori_loop(0, span - 1, step, (edge(xlow_ref), cells_at(0)))
    one(span - 1, before, here, edge(xhigh_ref))


def march(h, faces, xlow, xhigh, ylow, yhigh, crowding, last):
    rows, span, _, lanes = h.shape
    face = like((rows, span, lanes), h)
    count = 1 if last else 2
    operands = [h, *(faces or ()), xlow, xhigh, ylow[0], yhigh[0], crowding]
    return pl.pallas_call(
        functools.partial(march_kernel, faces is not None, last, ylow[1], yhigh[1]),
        in_specs=[VMEM] * len(operands),
        out_specs=[VMEM] * (1 + count),
        out_shape=[like(h.shape, h)] + [face] * count,
        input_output_aliases={0: 0},
        compiler_params=pltpu.CompilerParams(vmem_limit_bytes=2 * MIB),
        cost_estimate=pl.CostEstimate(flops=16 * h.size, bytes_accessed=12 * h.size, transcendentals=0),
        name="march",
    )(*operands)


def sums_kernel(h_ref, sum_ref):
    rows, span, depth, lanes = h_ref.shape
    sub = lax.broadcasted_iota(jnp.int32, (TILE, lanes), 0)

    def one(at, _):
        for row in range(rows):
            carry = None
            for t in range(depth // TILE):
                cells = h_ref[row, at, pl.ds(t * TILE, TILE), :]
                shift = 1
                while shift < TILE:
                    cells = cells + jnp.where(sub >= shift, pltpu.roll(cells, shift, 0), 0.0)
                    shift *= 2
                cells = cells if carry is None else cells + carry
                sum_ref[row, at, pl.ds(t * TILE, TILE), :] = cells
                carry = cells[TILE - 1 :]
        return 0

    lax.fori_loop(0, span, one, 0, unroll=2)


def running_sums(h):
    return pl.pallas_call(
        sums_kernel,
        in_specs=[VMEM],
        out_specs=VMEM,
        out_shape=like(h.shape, h),
        compiler_params=pltpu.CompilerParams(vmem_limit_bytes=2 * MIB),
        cost_estimate=pl.CostEstimate(flops=8 * h.size, bytes_accessed=8 * h.size, transcendentals=0),
        name="sums",
    )(h)


def ending_kernel(h_ref, low_ref, high_ref, end_ref, stage, sems):
    rows, span, depth, lanes = h_ref.shape
    tiles = depth // TILE
    chunk = span // CHUNKS
    sub = lax.broadcasted_iota(jnp.int32, (TILE, lanes), 0)

    def copy(k):
        return pltpu.make_async_copy(stage.at[k % SLOTS], end_ref.at[:, pl.ds(k * chunk, chunk)], sems.at[k])

    for k in range(CHUNKS):
        if k >= SLOTS:
            copy(k - SLOTS).wait()

        def one(step, _):
            at = step + k * chunk
            for row in range(rows):
                for t in range(tiles):
                    cells = h_ref[row, at, pl.ds(t * TILE, TILE), :]
                    if t == 0:
                        cells = cells + jnp.where(sub == 0, low_ref[row, pl.ds(at, 1), :], 0.0)
                    if t == tiles - 1:
                        cells = cells + jnp.where(sub == TILE - 1, high_ref[row, pl.ds(at, 1), :], 0.0)
                    stage[k % SLOTS, row, step, pl.ds(t * TILE, TILE), :] = cells
            return 0

        lax.fori_loop(0, chunk, one, 0, unroll=2)
        copy(k).start()
    for k in range(CHUNKS - SLOTS, CHUNKS):
        copy(k).wait()


def ending(h, low, high):
    rows, span, depth, lanes = h.shape
    return pl.pallas_call(
        ending_kernel,
        in_specs=[VMEM] * 3,
        out_specs=HBM,
        out_shape=like(h.shape, h),
        scratch_shapes=[pltpu.VMEM((SLOTS, rows, span // CHUNKS, depth, lanes), h.dtype), pltpu.SemaphoreType.DMA((CHUNKS,))],
        compiler_params=pltpu.CompilerParams(vmem_limit_bytes=8 * MIB),
        cost_estimate=pl.CostEstimate(flops=2 * h.size, bytes_accessed=8 * h.size, transcendentals=0),
        name="ending",
    )(h, low, high)


def relay_kernel(offset, got_ref, *refs):
    prior_ref, (own_ref, before_ref, next_ref) = refs[0], refs[-3:]
    rows = got_ref.shape[0]
    before = got_ref[...] if len(refs) == 3 else prior_ref[...] + got_ref[...]
    before_ref[...] = before
    next_ref[...] = before + own_ref[pl.ds(offset, rows)]


def relay(prior, got, own, part):
    operands = [got] + ([] if prior is None else [prior]) + [own]
    return pl.pallas_call(
        functools.partial(relay_kernel, part * got.shape[0]),
        in_specs=[VMEM] * len(operands),
        out_specs=[VMEM] * 2,
        out_shape=[like(got.shape, got)] * 2,
        compiler_params=pltpu.CompilerParams(vmem_limit_bytes=2 * MIB),
        cost_estimate=pl.CostEstimate(flops=2 * got.size, bytes_accessed=16 * got.size, transcendentals=0),
        name="relay",
    )(*operands)


def potential_kernel(scale, offset, given, sum_ref, got_ref, rest_ref, high_ref, *refs):
    prior_ref = refs[0] if given else None
    pot_ref, stage, sems = refs[-3:]
    rows, span, depth, lanes = stage.shape
    chunk = span // CHUNKS
    layer = lax.broadcasted_iota(jnp.int32, (depth, lanes), 0)

    def one(at, _):
        for row in range(rows):
            base = got_ref[row, pl.ds(at, 1), :]
            base = base if prior_ref is None else base + prior_ref[row, pl.ds(at, 1), :]
            base = base + rest_ref[row + offset, pl.ds(at, 1), :]
            high = high_ref[row + offset, pl.ds(at, 1), :]
            cells = sum_ref[row + offset, at] + base
            stage[row, at] = (cells + jnp.where(layer == depth - 1, high, 0.0)) * scale
        return 0

    copies = []
    for k in range(CHUNKS):
        lax.fori_loop(k * chunk, (k + 1) * chunk, one, 0, unroll=4)
        part = pl.ds(k * chunk, chunk)
        copies.append(pltpu.make_async_copy(stage.at[:, part], pot_ref.at[pl.ds(offset, rows), part], sems.at[k]))
        copies[-1].start()
    for copy in copies:
        copy.wait()


def potential(sums, prior, got, rest, high, scale, part, made):
    _, span, depth, lanes = sums.shape
    some = got.shape[0]
    operands = [sums, got, rest, high] + ([] if prior is None else [prior])
    return pl.pallas_call(
        functools.partial(potential_kernel, scale, part * some, prior is not None),
        in_specs=[VMEM] * len(operands) + [HBM] * (made is not None),
        out_specs=HBM,
        out_shape=like(sums.shape, sums),
        scratch_shapes=[pltpu.VMEM((some, span, depth, lanes), sums.dtype), pltpu.SemaphoreType.DMA((CHUNKS,))],
        input_output_aliases={} if made is None else {len(operands): 0},
        compiler_params=pltpu.CompilerParams(vmem_limit_bytes=(2 + 8 // PARTS) * MIB),
        cost_estimate=pl.CostEstimate(flops=2 * sums.size, bytes_accessed=8 * sums.size // PARTS, transcendentals=0),
        name="potential",
    )(*operands, *(() if made is None else (made,)))


def side_halos(both, first, final):
    lats, lons = lax.axis_size("lat"), lax.axis_size("lon")
    if lats == 2:
        swapped = lax.ppermute(both, "lat", [(0, 1), (1, 0)])
        ylow, yhigh = (swapped, 1), (swapped, 0)
    else:
        ylow = (lax.ppermute(both[1:], "lat", ups(lats)), 0)
        yhigh = (lax.ppermute(both[:1], "lat", downs(lats)), 0)
    xlow = lax.ppermute(final, "lon", ups(lons))
    xhigh = lax.ppermute(first, "lon", downs(lons))
    return xlow, xhigh, ylow, yhigh


def edges(h, low, high):
    rows, span = h.shape[:2]
    both = jnp.stack([add_faces(h[y], low[y], high[y]) for y in (0, rows - 1)])
    first, final = (add_faces(h[:, x], low[:, x], high[:, x]) for x in (0, span - 1))
    return both, first, final


def steps(field, crowding):
    levs = lax.axis_size("lev")
    depth = field.shape[2]
    faces = None
    h, both, first, final, ground = peel(field)
    low, high = layers(field)
    raw_low, raw_high = low, high
    for step in range(STEPS):
        last = step == STEPS - 1
        below = lax.ppermute(raw_high, "lev", ups(levs))
        above = lax.ppermute(raw_low, "lev", downs(levs))
        if step:
            below, above = below + 0.1 * older[0], above + 0.1 * older[1]
        halos = side_halos(both, first, final)
        outs = march(h, faces, *halos, crowding, last)
        h, older = outs[0], (low, high)
        if not last:
            raw_low, raw_high = outs[1], outs[2]
            low, high = raw_low + 0.1 * below, raw_high + 0.1 * above
            faces = (low, high)
            both, first, final = edges(h, low, high)
    rest = 0.1 * jnp.where(ground > 0.0, below, low)
    own = outs[1] + 0.1 * high + rest
    top = 0.1 * above
    sums = running_sums(h)
    field_end = ending(h, 0.1 * below, top)
    rows = own.shape[0] // PARTS
    nexts = [own[part * rows : (part + 1) * rows] for part in range(PARTS)]
    befores, gots = [None] * PARTS, [jnp.zeros_like(one) for one in nexts]
    for hop in range(levs - 1):
        for part in range(PARTS):
            if hop:
                befores[part], nexts[part] = relay(befores[part], gots[part], own, part)
            gots[part] = lax.ppermute(nexts[part], "lev", [(hop, hop + 1)])
    made = None
    for part in range(PARTS):
        made = potential(sums, befores[part], gots[part], rest, top, 1.0 / (depth * levs), part, made)
    return made, field_end


def solution(mesh):
    return jax.shard_map(
        steps,
        mesh=mesh,
        in_specs=(P("lat", "lon", "lev", None), P("lat", "lon", "lev", None)),
        out_specs=(P("lat", "lon", "lev", None), P("lat", "lon", "lev", None)),
        check_vma=False,
    )
```

```python
import functools

import jax
import jax.numpy as jnp
from jax import lax
from jax.experimental import pallas as pl
from jax.experimental.pallas import tpu as pltpu
from jax.sharding import PartitionSpec as P

STEPS = 4
TILE = 8
PARTS = 4
MIB = 1024 * 1024


CHUNKS = 8
GRANT = 40
SLOTS = 8
VMEM = pl.BlockSpec(memory_space=pltpu.VMEM)
HBM = pl.BlockSpec(memory_space=pltpu.HBM)


def ups(count):
    return [(i, (i + 1) % count) for i in range(count)]


def downs(count):
    return [((i + 1) % count, i) for i in range(count)]


def like(shape, array):
    return jax.ShapeDtypeStruct(shape, array.dtype)


def add_faces(cells, low, high):
    depth = cells.shape[-2]
    layer = lax.broadcasted_iota(jnp.int32, cells.shape, cells.ndim - 2)
    cells = jnp.where(layer == 0, jnp.expand_dims(low, -2), cells)
    return jnp.where(layer == depth - 1, jnp.expand_dims(high, -2), cells)


def layer_kernel(layer, f_ref, face_ref, sems):
    rows = f_ref.shape[0]
    copies = []
    for row in range(rows):
        copies.append(pltpu.make_async_copy(f_ref.at[row, :, layer], face_ref.at[row], sems.at[row]))
        copies[-1].start()
    for copy in copies:
        copy.wait()


def z_layer(field, layer):
    rows, span, _, lanes = field.shape
    return pl.pallas_call(
        functools.partial(layer_kernel, layer),
        in_specs=[HBM],
        out_specs=VMEM,
        out_shape=like((rows, span, lanes), field),
        scratch_shapes=[pltpu.SemaphoreType.DMA((rows,))],
        compiler_params=pltpu.CompilerParams(vmem_limit_bytes=50 * MIB),
        cost_estimate=pl.CostEstimate(flops=field.size, bytes_accessed=field.size, transcendentals=0),
        name="layer",
    )(field)


def peel_kernel(f_ref, h_ref, both_ref, first_ref, final_ref, ground_ref, sems):
    ground_ref[...] = jnp.full(ground_ref.shape, jnp.where(lax.axis_index("lev") == 0, 1.0, 0.0), ground_ref.dtype)
    rows, span, _, _ = h_ref.shape
    chunk = span // CHUNKS
    copies = []
    for k in range(CHUNKS):
        part = pl.ds(k * chunk, chunk)
        copies.append(pltpu.make_async_copy(f_ref.at[:, part], h_ref.at[:, part], sems.at[k]))
        copies[-1].start()

    def one(at, _):
        both_ref[0, at] = h_ref[0, at]
        both_ref[1, at] = h_ref[rows - 1, at]
        return 0

    for k in range(CHUNKS):
        copies[k].wait()
        lax.fori_loop(k * chunk, (k + 1) * chunk, one, 0, unroll=4)
    for row in range(rows):
        first_ref[row] = h_ref[row, 0]
        final_ref[row] = h_ref[row, span - 1]


def peel(field):
    rows, span, depth, lanes = field.shape
    edge = like((rows, depth, lanes), field)
    return pl.pallas_call(
        peel_kernel,
        in_specs=[HBM],
        out_specs=[VMEM] * 5,
        out_shape=[like(field.shape, field), like((2, span, depth, lanes), field), edge, edge, like((1, 1, lanes), field)],
        scratch_shapes=[pltpu.SemaphoreType.DMA((CHUNKS,))],
        compiler_params=pltpu.CompilerParams(vmem_limit_bytes=GRANT * MIB),
        cost_estimate=pl.CostEstimate(flops=4 * field.size, bytes_accessed=field.size, transcendentals=0),
        name="peel",
    )(field)


def march_kernel(fixed, last, ylow_at, yhigh_at, *refs):
    refs = list(refs)
    h_ref = refs.pop(0)
    low_ref, high_ref = (refs.pop(0), refs.pop(0)) if fixed else (None, None)
    xlow_ref, xhigh_ref, ylow_ref, yhigh_ref, c_ref, out_ref = refs[:6]
    refs = refs[6:]
    rows, span, depth, lanes = h_ref.shape
    tiles = depth // TILE
    sub = lax.broadcasted_iota(jnp.int32, (TILE, lanes), 0)
    first, final = sub == 0, sub == TILE - 1

    def tile(t):
        return pl.ds(t * TILE, TILE)

    def cells_at(at):
        out = []
        for row in range(rows):
            cells = [h_ref[row, at, tile(t), :] for t in range(tiles)]
            if fixed:
                cells[0] = jnp.where(first, low_ref[row, pl.ds(at, 1), :], cells[0])
                cells[-1] = jnp.where(final, high_ref[row, pl.ds(at, 1), :], cells[-1])
            out.append(cells)
        return out

    def edge(ref):
        return [[ref[row, tile(t), :] for t in range(tiles)] for row in range(rows)]

    def one(at, before, here, after):
        for row in range(rows):
            mids = here[row]
            down = [pltpu.roll(m, 1, 0) for m in mids]
            up = [pltpu.roll(m, TILE - 1, 0) for m in mids]
            news = []
            for t in range(tiles):
                ylow = ylow_ref[ylow_at, at, tile(t), :] if row == 0 else here[row - 1][t]
                yhigh = yhigh_ref[yhigh_at, at, tile(t), :] if row == rows - 1 else here[row + 1][t]
                around = (ylow + yhigh) + (before[row][t] + after[row][t])
                around = around + jnp.where(first, down[t - 1] if t else 0.0, down[t])
                around = around + jnp.where(final, up[t + 1] if t < tiles - 1 else 0.0, up[t])
                mid = mids[t]
                new = mid * (0.6 - 0.2 * (mid * c_ref[row, at, tile(t), :])) + 0.1 * around
                out_ref[row, at, tile(t), :] = new
                news.append(new)
            if last:
                total = functools.reduce(jnp.add, news)
                refs[0][row, pl.ds(at, 1), :] = jnp.sum(total, axis=0, keepdims=True)
            else:
                refs[0][row, pl.ds(at, 1), :] = news[0][:1]
                refs[1][row, pl.ds(at, 1), :] = news[-1][TILE - 1 :]

    def step(at, carry):
        before, here = carry
        after = cells_at(at + 1)
        one(at, before, here, after)
        return here, after

    before, here = lax.fori_loop(0, span - 1, step, (edge(xlow_ref), cells_at(0)))
    one(span - 1, before, here, edge(xhigh_ref))


def march(h, faces, xlow, xhigh, ylow, yhigh, crowding, last):
    rows, span, _, lanes = h.shape
    face = like((rows, span, lanes), h)
    count = 1 if last else 2
    operands = [h, *(faces or ()), xlow, xhigh, ylow[0], yhigh[0], crowding]
    return pl.pallas_call(
        functools.partial(march_kernel, faces is not None, last, ylow[1], yhigh[1]),
        in_specs=[VMEM] * len(operands),
        out_specs=[VMEM] * (1 + count),
        out_shape=[like(h.shape, h)] + [face] * count,
        input_output_aliases={0: 0},
        compiler_params=pltpu.CompilerParams(vmem_limit_bytes=2 * MIB),
        cost_estimate=pl.CostEstimate(flops=16 * h.size, bytes_accessed=12 * h.size, transcendentals=0),
        name="march",
    )(*operands)


def sums_kernel(h_ref, sum_ref):
    rows, span, depth, lanes = h_ref.shape
    sub = lax.broadcasted_iota(jnp.int32, (TILE, lanes), 0)

    def one(at, _):
        for row in range(rows):
            carry = None
            for t in range(depth // TILE):
                cells = h_ref[row, at, pl.ds(t * TILE, TILE), :]
                shift = 1
                while shift < TILE:
                    cells = cells + jnp.where(sub >= shift, pltpu.roll(cells, shift, 0), 0.0)
                    shift *= 2
                cells = cells if carry is None else cells + carry
                sum_ref[row, at, pl.ds(t * TILE, TILE), :] = cells
                carry = cells[TILE - 1 :]
        return 0

    lax.fori_loop(0, span, one, 0, unroll=2)


def running_sums(h):
    return pl.pallas_call(
        sums_kernel,
        in_specs=[VMEM],
        out_specs=VMEM,
        out_shape=like(h.shape, h),
        compiler_params=pltpu.CompilerParams(vmem_limit_bytes=2 * MIB),
        cost_estimate=pl.CostEstimate(flops=8 * h.size, bytes_accessed=8 * h.size, transcendentals=0),
        name="sums",
    )(h)


def ending_kernel(h_ref, low_ref, high_ref, end_ref, stage, sems):
    rows, span, depth, lanes = h_ref.shape
    tiles = depth // TILE
    chunk = span // CHUNKS
    sub = lax.broadcasted_iota(jnp.int32, (TILE, lanes), 0)

    def copy(k):
        return pltpu.make_async_copy(stage.at[k % SLOTS], end_ref.at[:, pl.ds(k * chunk, chunk)], sems.at[k])

    for k in range(CHUNKS):
        if k >= SLOTS:
            copy(k - SLOTS).wait()

        def one(group, _):
            start = pl.multiple_of(group * TILE, TILE)
            some = pl.ds(pl.multiple_of(start + k * chunk, TILE), TILE)
            for row in range(rows):
                low, high = low_ref[row, some, :], high_ref[row, some, :]
                for j in range(TILE):
                    for t in range(tiles):
                        cells = h_ref[row, k * chunk + start + j, pl.ds(t * TILE, TILE), :]
                        if t == 0:
                            cells = cells + jnp.where(sub == 0, low[j : j + 1], 0.0)
                        if t == tiles - 1:
                            cells = cells + jnp.where(sub == TILE - 1, high[j : j + 1], 0.0)
                        stage[k % SLOTS, row, start + j, pl.ds(t * TILE, TILE), :] = cells
            return 0

        lax.fori_loop(0, chunk // TILE, one, 0)
        copy(k).start()
    for k in range(CHUNKS - SLOTS, CHUNKS):
        copy(k).wait()


def ending(h, low, high):
    rows, span, depth, lanes = h.shape
    return pl.pallas_call(
        ending_kernel,
        in_specs=[VMEM] * 3,
        out_specs=HBM,
        out_shape=like(h.shape, h),
        scratch_shapes=[pltpu.VMEM((SLOTS, rows, span // CHUNKS, depth, lanes), h.dtype), pltpu.SemaphoreType.DMA((CHUNKS,))],
        compiler_params=pltpu.CompilerParams(vmem_limit_bytes=11 * MIB),
        cost_estimate=pl.CostEstimate(flops=2 * h.size, bytes_accessed=8 * h.size, transcendentals=0),
        name="ending",
    )(h, low, high)


def relay_kernel(offset, got_ref, *refs):
    prior_ref, (own_ref, before_ref, next_ref) = refs[0], refs[-3:]
    rows = got_ref.shape[0]
    before = got_ref[...] if len(refs) == 3 else prior_ref[...] + got_ref[...]
    before_ref[...] = before
    next_ref[...] = before + own_ref[pl.ds(offset, rows)]


def relay(prior, got, own, part):
    operands = [got] + ([] if prior is None else [prior]) + [own]
    return pl.pallas_call(
        functools.partial(relay_kernel, part * got.shape[0]),
        in_specs=[VMEM] * len(operands),
        out_specs=[VMEM] * 2,
        out_shape=[like(got.shape, got)] * 2,
        compiler_params=pltpu.CompilerParams(vmem_limit_bytes=2 * MIB),
        cost_estimate=pl.CostEstimate(flops=2 * got.size, bytes_accessed=16 * got.size, transcendentals=0),
        name="relay",
    )(*operands)


def potential_kernel(scale, offset, given, sum_ref, got_ref, rest_ref, high_ref, *refs):
    prior_ref = refs[0] if given else None
    pot_ref, stage, sems = refs[-3:]
    rows, span, depth, lanes = stage.shape
    chunk = span // CHUNKS
    final = lax.broadcasted_iota(jnp.int32, (TILE, lanes), 0) == TILE - 1
    tiles = depth // TILE

    def one(group, _):
        start = pl.multiple_of(group * TILE, TILE)
        some = pl.ds(start, TILE)
        for row in range(rows):
            base = got_ref[row, some, :] + rest_ref[row + offset, some, :]
            base = base if prior_ref is None else base + prior_ref[row, some, :]
            high = high_ref[row + offset, some, :]
            for j in range(TILE):
                for t in range(tiles):
                    cells = sum_ref[row + offset, start + j, pl.ds(t * TILE, TILE), :] + base[j : j + 1]
                    if t == tiles - 1:
                        cells = cells + jnp.where(final, high[j : j + 1], 0.0)
                    stage[row, start + j, pl.ds(t * TILE, TILE), :] = cells * scale
        return 0

    copies = []
    for k in range(CHUNKS):
        lax.fori_loop(k * chunk // TILE, (k + 1) * chunk // TILE, one, 0)
        part = pl.ds(k * chunk, chunk)
        copies.append(pltpu.make_async_copy(stage.at[:, part], pot_ref.at[pl.ds(offset, rows), part], sems.at[k]))
        copies[-1].start()
    for copy in copies:
        copy.wait()


def potential(sums, prior, got, rest, high, scale, part, made):
    _, span, depth, lanes = sums.shape
    some = got.shape[0]
    operands = [sums, got, rest, high] + ([] if prior is None else [prior])
    return pl.pallas_call(
        functools.partial(potential_kernel, scale, part * some, prior is not None),
        in_specs=[VMEM] * len(operands) + [HBM] * (made is not None),
        out_specs=HBM,
        out_shape=like(sums.shape, sums),
        scratch_shapes=[pltpu.VMEM((some, span, depth, lanes), sums.dtype), pltpu.SemaphoreType.DMA((CHUNKS,))],
        input_output_aliases={} if made is None else {len(operands): 0},
        compiler_params=pltpu.CompilerParams(vmem_limit_bytes=(2 + 8 // PARTS) * MIB),
        cost_estimate=pl.CostEstimate(flops=2 * sums.size, bytes_accessed=8 * sums.size // PARTS, transcendentals=0),
        name="potential",
    )(*operands, *(() if made is None else (made,)))


def side_halos(both, first, final):
    lats, lons = lax.axis_size("lat"), lax.axis_size("lon")
    if lats == 2:
        swapped = lax.ppermute(both, "lat", [(0, 1), (1, 0)])
        ylow, yhigh = (swapped, 1), (swapped, 0)
    else:
        ylow = (lax.ppermute(both[1:], "lat", ups(lats)), 0)
        yhigh = (lax.ppermute(both[:1], "lat", downs(lats)), 0)
    xlow = lax.ppermute(final, "lon", ups(lons))
    xhigh = lax.ppermute(first, "lon", downs(lons))
    return xlow, xhigh, ylow, yhigh


def edges(h, low, high):
    rows, span = h.shape[:2]
    both = jnp.stack([add_faces(h[y], low[y], high[y]) for y in (0, rows - 1)])
    first, final = (add_faces(h[:, x], low[:, x], high[:, x]) for x in (0, span - 1))
    return both, first, final


def steps(field, crowding):
    levs = lax.axis_size("lev")
    depth = field.shape[2]
    faces = None
    h, both, first, final, ground = peel(field)
    high = z_layer(field, depth - 1)
    low = z_layer(field, 0)
    raw_low, raw_high = low, high
    for step in range(STEPS):
        last = step == STEPS - 1
        below = lax.ppermute(raw_high, "lev", ups(levs))
        above = lax.ppermute(raw_low, "lev", downs(levs))
        if step:
            below, above = below + 0.1 * older[0], above + 0.1 * older[1]
        halos = side_halos(both, first, final)
        outs = march(h, faces, *halos, crowding, last)
        h, older = outs[0], (low, high)
        if not last:
            raw_low, raw_high = outs[1], outs[2]
            low, high = raw_low + 0.1 * below, raw_high + 0.1 * above
            faces = (low, high)
            both, first, final = edges(h, low, high)
    rest = 0.1 * jnp.where(ground > 0.0, below, low)
    own = outs[1] + 0.1 * high + rest
    top = 0.1 * above
    sums = running_sums(h)
    field_end = ending(h, 0.1 * below, top)
    rows = own.shape[0] // PARTS
    nexts = [own[part * rows : (part + 1) * rows] for part in range(PARTS)]
    befores, gots = [None] * PARTS, [jnp.zeros_like(one) for one in nexts]
    for hop in range(levs - 1):
        for part in range(PARTS):
            if hop:
                befores[part], nexts[part] = relay(befores[part], gots[part], own, part)
            gots[part] = lax.ppermute(nexts[part], "lev", [(hop, hop + 1)])
    made = None
    for part in range(PARTS):
        made = potential(sums, befores[part], gots[part], rest, top, 1.0 / (depth * levs), part, made)
    return made, field_end


def solution(mesh):
    return jax.shard_map(
        steps,
        mesh=mesh,
        in_specs=(P("lat", "lon", "lev", None), P("lat", "lon", "lev", None)),
        out_specs=(P("lat", "lon", "lev", None), P("lat", "lon", "lev", None)),
        check_vma=False,
    )
```
